64 devices in a mesh: dp: 8 (over x, y, core), sp: 8 (over z).
Axes of the slice: x: 2, y: 2, z: 8, core: 2. Of those that a mesh axis runs over, the one named last changes fastest.
The devices are a block of a 4x4x8 slice.
Arguments:
- x: bfloat16 [8192, 8192], P(('dp', 'sp')), parts along dimension 0
- gain: bfloat16 [8192], replicated
- wq: bfloat16 [8192, 8192], replicated
- wk: bfloat16 [8192, 8192], replicated
- wv: bfloat16 [8192, 8192], replicated
- wo: bfloat16 [8192, 8192], replicated
Outputs:
- output: bfloat16 [8192, 8192], P(('dp', 'sp')), parts along dimension 0
There are 8 independent parts. The reference program is written for one: setup_inputs(seed, part) draws one part's arguments, and reference() takes and returns one part's arrays. A program takes and returns all parts, laid end to end along the dimension named above; an argument that names none is the same for every part.
All inputs are finite; a program needn't handle non-finite values.
Results may differ from the reference program's by a relative error of at most 0.012.
Values are sent between devices in bfloat16 or wider.
A program may use at most 768 MiB of HBM per device.

```python
import jax
import jax.numpy as jnp
from jax import lax

ROWS = 1024
D = 8192
HEADS = 64
KV_HEADS = 64
HEAD = 128
THETA = 10000


def setup_inputs(seed: int = 0, part: int = 0) -> dict:
    kx, kn, kq, kk, kv, ko = jax.random.split(jax.random.key(seed), 6)

    def weights(key, rows, columns):
        return jax.random.normal(key, (rows, columns), jnp.float32) * rows**-0.5

    drawn = {
        "x": jax.random.normal(jax.random.fold_in(kx, part), (ROWS, D), jnp.float32),
        "gain": 1 + 0.1 * jax.random.normal(kn, (D,), jnp.float32),
        "wq": 2 * weights(kq, D, HEADS * HEAD),
        "wk": 2 * weights(kk, D, KV_HEADS * HEAD),
        "wv": 4 * weights(kv, D, KV_HEADS * HEAD),
        "wo": weights(ko, HEADS * HEAD, D),
    }
    return {k: v.astype(jnp.bfloat16) for k, v in drawn.items()}


def normed(x, gain):
    wide = x.astype(jnp.float32)
    scale = lax.rsqrt(jnp.mean(wide * wide, -1, keepdims=True) + 1e-6)
    return (wide * scale * gain.astype(jnp.float32)).astype(jnp.bfloat16)


def turned(t, place, theta):
    half = t.shape[-1] // 2
    angle = place.astype(jnp.float32)[:, None] * theta ** (-jnp.arange(half, dtype=jnp.float32) / half)
    cos, sin = jnp.cos(angle)[:, None], jnp.sin(angle)[:, None]
    a, b = t[..., :half].astype(jnp.float32), t[..., half:].astype(jnp.float32)
    return jnp.concatenate([a * cos - b * sin, b * cos + a * sin], -1).astype(jnp.bfloat16)


def matmul(a, w):
    return jnp.dot(a, w, preferred_element_type=jnp.float32).astype(jnp.bfloat16)


def einsum(form, a, b):
    return jnp.einsum(form, a.astype(jnp.float32), b.astype(jnp.float32))


def attention(q, k, v):
    scores = einsum("tgsd,ugd->gstu", q, k) * q.shape[-1] ** -0.5
    token = jnp.arange(q.shape[0])
    scores = jnp.where(token[:, None] >= token, scores, -jnp.inf)
    weights = jax.nn.softmax(scores, -1).astype(jnp.bfloat16)
    return einsum("gstu,ugd->tgsd", weights, v).astype(jnp.bfloat16)


def reference(x, gain, wq, wk, wv, wo):
    a, place = normed(x, gain), jnp.arange(ROWS)
    q = turned(matmul(a, wq).reshape(ROWS, HEADS, HEAD), place, THETA).reshape(ROWS, KV_HEADS, -1, HEAD)
    k = turned(matmul(a, wk).reshape(ROWS, KV_HEADS, HEAD), place, THETA)
    v = matmul(a, wv).reshape(ROWS, KV_HEADS, HEAD)
    seen = attention(q, k, v).reshape(ROWS, HEADS * HEAD)
    return (x.astype(jnp.float32) + jnp.dot(seen, wo, preferred_element_type=jnp.float32)).astype(jnp.bfloat16)
```

```python
import functools

import jax
import jax.numpy as jnp
from jax import lax
from jax.experimental import pallas as pl
from jax.experimental.pallas import tpu as pltpu
from jax.sharding import PartitionSpec as P

HEAD = 128
THETA = 10000
LOG2E = 1.4426950408889634
HIDDEN = -1e30
SLOTS = 3
WO_SLOTS = 3
AHEAD = 24
RUNS = 2
VMEM = 67_000_000


def _dot(a, b, ca=1, cb=0):
    return lax.dot_general(a, b, (((ca,), (cb,)), ((), ())), preferred_element_type=jnp.float32)


def _kernel(n, own, x_ref, gain_ref, cos_ref, sin_ref, wq_ref, wk_ref, wv_ref, wo_ref, out_ref,
            xs, a, wbuf, stage, recv, ostage, obuf, wobuf, acc, ybuf,
            x_sems, w_sem, wo_sem, send_sem, recv_sem, osend_sem, orecv_sem, fsend_sem, frecv_sem, y_sems):
    d = x_ref.shape[1]
    half = d // 2
    bn = wbuf.shape[2]
    owner_span = wq_ref.shape[1] // n
    core_span = owner_span // 2
    me = lax.axis_index("sp")
    dp = lax.axis_index("dp")
    c = lax.rem(dp, 2)
    mate = dp + 1 - 2 * c
    blocks = RUNS * 3 * n

    def off(i):
        e = lax.rem(i, 2)
        k = lax.div(i, 2)
        return (1 - e) * (n // 2 - k) + e * (n // 2 + 1 + k)

    def parts(b):
        p = lax.div(b, 3 * n)
        w = lax.div(lax.rem(b, 3 * n), n)
        i = lax.rem(b, n)
        return p, w, i, lax.rem(me + off(i), n)

    rows4 = d // 4

    def w_start(b):
        p, w, _, to = parts(b)
        col = pl.multiple_of(to * owner_span + c * core_span + p * bn, bn)
        slot = lax.rem(b, SLOTS)
        for k, ref in enumerate((wq_ref, wk_ref, wv_ref)):
            @pl.when(w == k)
            def _():
                for r in range(4):
                    pltpu.make_async_copy(ref.at[pl.ds(r * rows4, rows4), pl.ds(col, bn)],
                                          wbuf.at[slot, pl.ds(r * rows4, rows4), :], w_sem.at[slot]).start()

    def w_wait(b):
        slot = lax.rem(b, SLOTS)
        pltpu.make_async_copy(wq_ref.at[:, pl.ds(0, bn)], wbuf.at[slot], w_sem.at[slot]).wait()

    def send(b):
        p, w, _, to = parts(b)
        at = (p * 3 + w) * n + me
        return pltpu.make_async_remote_copy(stage.at[b], recv.at[at], send_sem.at[b], recv_sem.at[at], device_id={"sp": to},
                                            device_id_type=pl.DeviceIdType.MESH)

    for b in range(SLOTS):
        w_start(jnp.int32(b))
    mine = pltpu.make_async_copy(x_ref, xs.at[c], x_sems.at[0])
    mine.start()
    barrier = pltpu.get_barrier_semaphore()
    for s in range(1, n):
        pl.semaphore_signal(barrier, inc=1, device_id={"sp": lax.rem(me + s, n)}, device_id_type=pl.DeviceIdType.MESH)
    pl.semaphore_signal(barrier, inc=1, device_id={"dp": mate}, device_id_type=pl.DeviceIdType.MESH)
    pl.semaphore_wait(barrier, n)
    swap = pltpu.make_async_remote_copy(x_ref, xs.at[c], x_sems.at[1], x_sems.at[2], device_id={"dp": mate},
                                        device_id_type=pl.DeviceIdType.MESH)
    swap.start()

    def norm(g):
        def strip(r, _):
            at = pl.multiple_of(r * 16, 16)
            wide = xs[g, pl.ds(at, 16), :].astype(jnp.float32)
            scale = lax.rsqrt(jnp.mean(wide * wide, -1, keepdims=True) + 1e-6)
            a[pl.ds(pl.multiple_of(g * own + at, 16), 16), :] = (wide * scale * gain_ref[...].astype(jnp.float32)).astype(jnp.bfloat16)
        lax.fori_loop(0, own // 16, strip, None)

    mine.wait()
    norm(c)
    swap.wait_recv()
    norm(1 - c)

    def project(b, _):
        p, w, i, to = parts(b)
        slot = lax.rem(b, SLOTS)
        w_wait(b)

        @pl.when((b >= 1) & (lax.rem(b - 1, n) != n - 1))
        def _():
            send(b - 1).start()

        @pl.when((b >= AHEAD) & (lax.rem(b - AHEAD, n) != n - 1))
        def _():
            send(b - AHEAD).wait_send()

        t = _dot(a[...], wbuf[slot]).astype(jnp.bfloat16).astype(jnp.float32)

        @pl.when(b + SLOTS < blocks)
        def _():
            w_start(b + SLOTS)

        turn = w < 2
        cos = jnp.where(turn, cos_ref[...], 1.0)
        sin = sin_ref[...]
        pieces = []
        for g in range(2):
            line = []
            for h in range(bn // HEAD):
                u = t[g * own : (g + 1) * own, h * HEAD : (h + 1) * HEAD]
                turned = u * cos + pltpu.roll(u, HEAD // 2, 1) * sin
                line.append(jnp.where(turn, turned, u).astype(jnp.bfloat16))
            pieces.append(jnp.concatenate(line, axis=1))
        block = jnp.concatenate(pieces, axis=0)

        @pl.when(i != n - 1)
        def _():
            stage[b] = block

        @pl.when(i == n - 1)
        def _():
            recv[(p * 3 + w) * n + me] = block

    lax.fori_loop(0, blocks, project, None)

    def source(i):
        return lax.rem(me + n - lax.rem(off(lax.rem(i + n - 1, n)), n), n)

    def wo_start(t):
        p, src = lax.div(t, n), source(lax.rem(t, n))
        slot = lax.rem(t, WO_SLOTS)
        for k in range(2):
            row = pl.multiple_of(src * owner_span + k * core_span + p * bn, bn)
            pltpu.make_async_copy(wo_ref.at[pl.ds(row, bn), pl.ds(pl.multiple_of(c * half, half), half)],
                                  wobuf.at[slot, pl.ds(k * bn, bn), :], wo_sem.at[slot]).start()

    for t in range(WO_SLOTS):
        wo_start(jnp.int32(t))

    def osend(p, to):
        return pltpu.make_async_remote_copy(ostage.at[p * n + to], obuf.at[p, me, c], osend_sem.at[p * n + to],
                                            orecv_sem.at[p * n + me], device_id={"sp": to}, device_id_type=pl.DeviceIdType.MESH)

    e = HEAD**-0.5 * LOG2E
    wide = 2 * own

    def attention(p, _):
        def arrive(s, _):
            src = lax.rem(me + s, n)
            for w in range(3):
                at = (p * 3 + w) * n + src
                pltpu.make_async_remote_copy(stage.at[0], recv.at[at], send_sem.at[0], recv_sem.at[at], device_id={"sp": me},
                                             device_id_type=pl.DeviceIdType.MESH).wait_recv()
        lax.fori_loop(1, n, arrive, None)

        def head(gh, _):
            g, h = lax.div(gh, bn // HEAD), lax.rem(gh, bn // HEAD)
            r, l = pl.ds(pl.multiple_of(g * own, own), own), pl.ds(pl.multiple_of(h * HEAD, HEAD), HEAD)
            for jj in range(n // 2):
                q = recv[pl.ds((p * 3) * n + 2 * jj, 2), r, l].reshape(wide, HEAD)
                keys = (jj + 1) * wide
                k = recv[pl.ds((p * 3 + 1) * n, 2 * jj + 2), r, l].reshape(keys, HEAD)
                v = recv[pl.ds((p * 3 + 2) * n, 2 * jj + 2), r, l].reshape(keys, HEAD)
                s = _dot(k, q, 1, 1)
                ok = lax.broadcasted_iota(jnp.int32, (wide, wide), 1) >= lax.broadcasted_iota(jnp.int32, (wide, wide), 0)
                edge = jnp.where(ok, s[keys - wide :, :], HIDDEN)
                s = edge if jj == 0 else jnp.concatenate([s[: keys - wide, :], edge], axis=0)
                top = s.max(axis=0, keepdims=True)
                weights = jnp.exp2((s - top) * e)
                total = weights.sum(axis=0, keepdims=True)
                mix = _dot(v, weights.astype(jnp.bfloat16), 0, 0)
                o = (mix * (1 / total)).T.astype(jnp.bfloat16)
                ostage[pl.ds(p * n + 2 * jj, 2), r, l] = o.reshape(2, own, HEAD)
        lax.fori_loop(0, 2 * (bn // HEAD), head, None)
        obuf[p, me, c] = ostage[p * n + me]

        def give(i, _):
            osend(p, lax.rem(me + off(i), n)).start()
        lax.fori_loop(0, n - 1, give, None)

    lax.fori_loop(0, RUNS, attention, None)

    for g in range(2):
        acc[g * own : (g + 1) * own, :] = xs[g, :, pl.ds(pl.multiple_of(c * half, half), half)].astype(jnp.float32)

    def forward(t):
        p, src = lax.div(t, n), source(lax.rem(t, n))
        return pltpu.make_async_remote_copy(obuf.at[p, src, c], obuf.at[p, src, c], fsend_sem.at[t], frecv_sem.at[t],
                                            device_id={"dp": mate}, device_id_type=pl.DeviceIdType.MESH)

    steps = RUNS * n
    tile = min(512, half)

    def output(t, _):
        @pl.when(t < steps)
        def _():
            p, i = lax.div(t, n), lax.rem(t, n)

            @pl.when(i != 0)
            def _():
                src = source(i)
                pltpu.make_async_remote_copy(ostage.at[0], obuf.at[p, src, c], osend_sem.at[0], orecv_sem.at[p * n + src],
                                             device_id={"sp": me}, device_id_type=pl.DeviceIdType.MESH).wait_recv()
            forward(t).start()

        @pl.when(t > 0)
        def _():
            u = t - 1
            p, src = lax.div(u, n), source(lax.rem(u, n))
            slot = lax.rem(u, WO_SLOTS)
            pltpu.make_async_remote_copy(obuf.at[p, src, 1 - c], obuf.at[p, src, 1 - c], fsend_sem.at[u], frecv_sem.at[u],
                                         device_id={"dp": mate}, device_id_type=pl.DeviceIdType.MESH).wait_recv()
            pltpu.make_async_copy(wo_ref.at[pl.ds(0, 2 * bn), pl.ds(0, half)], wobuf.at[slot], wo_sem.at[slot]).wait()
            o = jnp.concatenate([obuf[p, src, 0], obuf[p, src, 1]], axis=1)

            def columns(k, _):
                here = pl.ds(pl.multiple_of(k * tile, tile), tile)
                acc[:, here] += _dot(o, wobuf[slot, :, here])
            lax.fori_loop(0, half // tile, columns, None)

            @pl.when(u + WO_SLOTS < steps)
            def _():
                wo_start(u + WO_SLOTS)

    lax.fori_loop(0, steps + 1, output, None)

    for g in range(2):
        ybuf[g] = acc[g * own : (g + 1) * own, :].astype(jnp.bfloat16)
    there = out_ref.at[:, pl.ds(pl.multiple_of(c * half, half), half)]
    give = pltpu.make_async_remote_copy(ybuf.at[1 - c], there, y_sems.at[0], y_sems.at[1], device_id={"dp": mate},
                                        device_id_type=pl.DeviceIdType.MESH)
    keep = pltpu.make_async_copy(ybuf.at[c], there, y_sems.at[2])
    give.start()
    keep.start()

    swap.wait_send()

    def left(b, _):
        @pl.when(lax.rem(b, n) != n - 1)
        def _():
            send(b).wait_send()
    lax.fori_loop(blocks - AHEAD, blocks, left, None)

    def oleft(k, _):
        @pl.when(lax.rem(k, n) != me)
        def _():
            osend(lax.div(k, n), lax.rem(k, n)).wait_send()
        forward(k).wait_send()
    lax.fori_loop(0, steps, oleft, None)
    give.wait_send()
    keep.wait()
    pltpu.make_async_remote_copy(ybuf.at[c], out_ref.at[:, pl.ds(pl.multiple_of((1 - c) * half, half), half)], y_sems.at[0], y_sems.at[1],
                                 device_id={"dp": mate}, device_id_type=pl.DeviceIdType.MESH).wait_recv()


def solution(mesh):
    n = mesh.shape["sp"]

    def step(x, gain, wq, wk, wv, wo):
        own, d = x.shape
        bn = wq.shape[1] // n // 2 // RUNS
        half = HEAD // 2
        place = lax.axis_index("sp") * own + jnp.arange(own)
        angle = place.astype(jnp.float32)[:, None] * THETA ** (-jnp.arange(half, dtype=jnp.float32) / half)
        cos, sin = jnp.cos(angle), jnp.sin(angle)
        cos, sin = jnp.concatenate([cos, cos], -1), jnp.concatenate([-sin, sin], -1)
        blocks, steps = RUNS * 3 * n, RUNS * n
        vmem = pl.BlockSpec(memory_space=pltpu.VMEM)
        hbm = pl.BlockSpec(memory_space=pl.ANY)
        dma, low = pltpu.SemaphoreType.DMA, jnp.bfloat16
        return pl.pallas_call(
            functools.partial(_kernel, n, own),
            out_shape=jax.ShapeDtypeStruct((own, d), low),
            in_specs=[hbm, vmem, vmem, vmem, hbm, hbm, hbm, hbm],
            out_specs=hbm,
            scratch_shapes=[
                pltpu.VMEM((2, own, d), low),
                pltpu.VMEM((2 * own, d), low),
                pltpu.VMEM((SLOTS, d, bn), low),
                pltpu.VMEM((blocks, 2 * own, bn), low),
                pltpu.VMEM((blocks, 2 * own, bn), low),
                pltpu.VMEM((steps, 2 * own, bn), low),
                pltpu.VMEM((RUNS, n, 2, 2 * own, bn), low),
                pltpu.VMEM((WO_SLOTS, 2 * bn, d // 2), low),
                pltpu.VMEM((2 * own, d // 2), jnp.float32),
                pltpu.VMEM((2, own, d // 2), low),
                dma((3,)), dma((SLOTS,)), dma((WO_SLOTS,)), dma((blocks,)), dma((blocks,)), dma((steps,)), dma((steps,)),
                dma((steps,)), dma((steps,)), dma((3,)),
            ],
            compiler_params=pltpu.CompilerParams(collective_id=0, has_side_effects=True, vmem_limit_bytes=VMEM),
        )(x, gain.reshape(1, d), cos, sin, wq, wk, wv, wo)

    tokens, whole = P(("dp", "sp"), None), P(None, None)
    return jax.shard_map(
        step,
        mesh=mesh,
        in_specs=(tokens, P(None), whole, whole, whole, whole),
        out_specs=tokens,
        check_vma=False,
    )
```

```python
import functools

import jax
import jax.numpy as jnp
from jax import lax
from jax.experimental import pallas as pl
from jax.experimental.pallas import tpu as pltpu
from jax.sharding import PartitionSpec as P

HEAD = 128
THETA = 10000
LOG2E = 1.4426950408889634
HIDDEN = -1e30
SLOTS = 3
WO_SLOTS = 3
AHEAD = 24
RUNS = 2
VMEM = 67_000_000


def _dot(a, b, ca=1, cb=0):
    return lax.dot_general(a, b, (((ca,), (cb,)), ((), ())), preferred_element_type=jnp.float32)


def _among(z, places):
    return functools.reduce(jnp.logical_or, [z == k for k in places])


def _kernel(n, own, x_ref, gain_ref, cos_ref, sin_ref, wq_ref, wk_ref, wv_ref, wo_ref, out_ref,
            xs, a, wbuf, stage, recv, ostage, obuf, wobuf, acc, ybuf, via,
            x_sems, w_sem, wo_sem, send_sem, recv_sem, osend_sem, orecv_sem, fsend_sem, frecv_sem, vsend_sem, vrecv_sem, y_sems):
    d = x_ref.shape[1]
    half = d // 2
    bn = wbuf.shape[2]
    owner_span = wq_ref.shape[1] // n
    core_span = owner_span // 2
    me = lax.axis_index("sp")
    dp = lax.axis_index("dp")
    c = lax.rem(dp, 2)
    mate = dp + 1 - 2 * c
    blocks = RUNS * 3 * n

    def off(i):
        e = lax.rem(i, 2)
        k = lax.div(i, 2)
        return (1 - e) * (n // 2 - k) + e * (n // 2 + 1 + k)

    def parts(b):
        p = lax.div(b, 3 * n)
        w = lax.div(lax.rem(b, 3 * n), n)
        i = lax.rem(b, n)
        return p, w, i, lax.rem(me + off(i), n)

    rows4 = d // 4

    def w_start(b):
        p, w, _, to = parts(b)
        col = pl.multiple_of(to * owner_span + c * core_span + p * bn, bn)
        slot = lax.rem(b, SLOTS)
        for k, ref in enumerate((wq_ref, wk_ref, wv_ref)):
            @pl.when(w == k)
            def _():
                for r in range(4):
                    pltpu.make_async_copy(ref.at[pl.ds(r * rows4, rows4), pl.ds(col, bn)],
                                          wbuf.at[slot, pl.ds(r * rows4, rows4), :], w_sem.at[slot]).start()

    def w_wait(b):
        slot = lax.rem(b, SLOTS)
        pltpu.make_async_copy(wq_ref.at[:, pl.ds(0, bn)], wbuf.at[slot], w_sem.at[slot]).wait()

    def remote(src, dst, one, two, **to):
        return pltpu.make_async_remote_copy(src, dst, one, two, device_id=to, device_id_type=pl.DeviceIdType.MESH)

    def upward(w, z):
        up_q, up_kv, up_o = (_among(z, k) for k in ((2, 3, 5, 6, 7), (2, 3, 6, 7), (6, 7)))
        return jnp.where(w == 0, up_q, jnp.where(w == 3, up_o, up_kv)) if not isinstance(w, int) else (up_q, up_kv, up_kv, up_o)[w]

    quarter = n // 4

    def sends(b):
        _, w, i, _ = parts(b)
        return (i != n - 1) & jnp.logical_not((w == 0) & (me == 0))

    def send(b, rows=slice(None)):
        p, w, i, to = parts(b)
        at = (p * 3 + w) * n + me
        return remote(stage.at[b, rows], recv.at[at, rows], send_sem.at[b], recv_sem.at[at], sp=to)

    def send_start(b, rows=slice(None)):
        p, w, i, to = parts(b)

        @pl.when(sends(b) & (i != 0))
        def _():
            send(b, rows).start()

        @pl.when(sends(b) & (i == 0))
        def _():
            up = upward(w, me).astype(jnp.int32)
            at = (p * 3 + w) * 2 + 1 - up
            remote(stage.at[b, rows], via.at[at, rows], send_sem.at[b], vrecv_sem.at[at],
                   sp=lax.rem(me + n - quarter + 2 * quarter * up, n)).start()

    def relay(p, w, result=False):
        group = RUNS * 3 + p if result else p * 3 + w
        for side in range(2):
            come = lax.rem(me + n - quarter + 2 * quarter * side, n)
            go = lax.rem(me + quarter + (n - 2 * quarter) * side, n)
            up = upward(3 if result else w, come)
            used = jnp.logical_not(up) if side else up
            used = used & (go != 0) if result else used & jnp.logical_not((w == 0) & (come == 0))
            at = group * 2 + side

            @pl.when(used)
            def _():
                remote(via.at[at], via.at[at], vsend_sem.at[at], vrecv_sem.at[at], sp=me).wait_recv()
                if result:
                    remote(via.at[at], obuf.at[p, come, c], vsend_sem.at[at], orecv_sem.at[p * n + come], sp=go).start()
                else:
                    to = (p * 3 + w) * n + come
                    remote(via.at[at], recv.at[to], vsend_sem.at[at], recv_sem.at[to], sp=go).start()

    def relayed(p, w, result=False):
        group = RUNS * 3 + p if result else p * 3 + w
        for side in range(2):
            come = lax.rem(me + n - quarter + 2 * quarter * side, n)
            go = lax.rem(me + quarter + (n - 2 * quarter) * side, n)
            up = upward(3 if result else w, come)
            used = jnp.logical_not(up) if side else up
            used = used & (go != 0) if result else used & jnp.logical_not((w == 0) & (come == 0))
            at = group * 2 + side

            @pl.when(used)
            def _():
                remote(via.at[at], via.at[at], vsend_sem.at[at], vrecv_sem.at[at], sp=me).wait_send()

    for b in range(SLOTS):
        w_start(jnp.int32(b))
    mine = pltpu.make_async_copy(x_ref, xs.at[c], x_sems.at[0])
    mine.start()
    barrier = pltpu.get_barrier_semaphore()
    for s in range(1, n):
        pl.semaphore_signal(barrier, inc=1, device_id={"sp": lax.rem(me + s, n)}, device_id_type=pl.DeviceIdType.MESH)
    pl.semaphore_signal(barrier, inc=1, device_id={"dp": mate}, device_id_type=pl.DeviceIdType.MESH)
    pl.semaphore_wait(barrier, n)
    swap = pltpu.make_async_remote_copy(x_ref, xs.at[c], x_sems.at[1], x_sems.at[2], device_id={"dp": mate},
                                        device_id_type=pl.DeviceIdType.MESH)
    swap.start()

    def norm(g):
        def strip(r, _):
            at = pl.multiple_of(r * 16, 16)
            wide = xs[g, pl.ds(at, 16), :].astype(jnp.float32)
            scale = lax.rsqrt(jnp.mean(wide * wide, -1, keepdims=True) + 1e-6)
            a[pl.ds(pl.multiple_of(g * own + at, 16), 16), :] = (wide * scale * gain_ref[...].astype(jnp.float32)).astype(jnp.bfloat16)
        lax.fori_loop(0, own // 16, strip, None)

    def turned(t, w, rows):
        turn = w < 2
        pieces = []
        for g in range(rows):
            line = []
            for h in range(bn // HEAD):
                u = t[g * own : (g + 1) * own, h * HEAD : (h + 1) * HEAD]
                u = jnp.where(turn, u * cos_ref[...] + pltpu.roll(u, HEAD // 2, 1) * sin_ref[...], u)
                line.append(u.astype(jnp.bfloat16))
            pieces.append(jnp.concatenate(line, axis=1))
        return jnp.concatenate(pieces, axis=0)

    mine.wait()
    norm(c)

    def early_rows(k):
        return pl.ds(pl.multiple_of(jnp.where(k < SLOTS, c, 1 - c) * own, own), own)

    def early(k, _):
        b, rows = lax.rem(k, SLOTS), early_rows(k)

        @pl.when(k < SLOTS)
        def _():
            w_wait(b)

        @pl.when(k == SLOTS)
        def _():
            remote(x_ref, xs.at[1 - c], x_sems.at[1], x_sems.at[2], dp=mate).wait_recv()
            norm(1 - c)

        @pl.when(k > 0)
        def _():
            send_start(lax.rem(k - 1, SLOTS), early_rows(k - 1))
        _, w, _, _ = parts(b)
        t = _dot(a[rows, :], wbuf[b]).astype(jnp.bfloat16).astype(jnp.float32)

        @pl.when(k >= SLOTS)
        def _():
            w_start(b + SLOTS)
        stage[b, rows, :] = turned(t, w, 1)

    lax.fori_loop(0, 2 * SLOTS, early, None)

    def project(b, _):
        p, w, i, to = parts(b)
        slot = lax.rem(b, SLOTS)
        w_wait(b)

        @pl.when(b == SLOTS)
        def _():
            send_start(b - 1, early_rows(2 * SLOTS - 1))

        @pl.when(b > SLOTS)
        def _():
            send_start(b - 1)

        @pl.when((b >= AHEAD) & sends(jnp.maximum(b - AHEAD, 0)))
        def _():
            send(b - AHEAD).wait_send()

        @pl.when((i == n // 2 - 1) & (b >= n))
        def _():
            before = lax.div(b, n) - 1
            relay(lax.div(before, 3), lax.rem(before, 3))

        t = _dot(a[...], wbuf[slot]).astype(jnp.bfloat16).astype(jnp.float32)

        @pl.when(b + SLOTS < blocks)
        def _():
            w_start(b + SLOTS)

        block = turned(t, w, 2)
        stage[b] = block

        @pl.when(i == n - 1)
        def _():
            recv[(p * 3 + w) * n + me] = block

    lax.fori_loop(SLOTS, blocks, project, None)

    def source(i):
        return lax.rem(me + n - lax.rem(off(jnp.where(i == 0, n - 1, jnp.where(i == n - 1, 0, i))), n), n)

    def wo_start(t):
        p, src = lax.div(t, n), source(lax.rem(t, n))
        slot = lax.rem(t, WO_SLOTS)
        for k in range(2):
            row = pl.multiple_of(src * owner_span + k * core_span + p * bn, bn)
            pltpu.make_async_copy(wo_ref.at[pl.ds(row, bn), pl.ds(pl.multiple_of(c * half, half), half)],
                                  wobuf.at[slot, pl.ds(k * bn, bn), :], wo_sem.at[slot]).start()

    for t in range(WO_SLOTS):
        wo_start(jnp.int32(t))

    relay(RUNS - 1, 2)

    def osend(p, to):
        return remote(ostage.at[p * n + to], obuf.at[p, me, c], osend_sem.at[p * n + to], orecv_sem.at[p * n + me], sp=to)

    e = HEAD**-0.5 * LOG2E

    def attend(q, k, v, first, last):
        s = _dot(k, q, 1, 1)
        queries = q.shape[0]
        shape = (last - first, queries)
        ok = lax.broadcasted_iota(jnp.int32, shape, 1) + (last - queries) >= lax.broadcasted_iota(jnp.int32, shape, 0) + first
        edge = jnp.where(ok, s[first:, :], HIDDEN)
        s = edge if first == 0 else jnp.concatenate([s[:first, :], edge], axis=0)
        top = s.max(axis=0, keepdims=True)
        weights = jnp.exp2((s - top) * e)
        total = weights.sum(axis=0, keepdims=True)
        mix = _dot(v, weights.astype(jnp.bfloat16), 0, 0)
        return (mix * (1 / total)).T.astype(jnp.bfloat16)

    def attention(p, _):
        @pl.when(me == 0)
        def _():
            def local(i, _):
                to = lax.rem(off(i), n)
                for g in range(2):
                    for h in range(bn // HEAD):
                        q, k, v = (stage[(p * 3 + w) * n + i, g * own : (g + 1) * own, h * HEAD : (h + 1) * HEAD] for w in range(3))
                        obuf[p, to, c, g * own : (g + 1) * own, h * HEAD : (h + 1) * HEAD] = attend(q, k, v, 0, own)
            lax.fori_loop(0, n, local, None)

        def arrive(s, _):
            src = lax.rem(me + s, n)
            for w in range(3):
                at = (p * 3 + w) * n + src

                @pl.when(jnp.logical_not((w == 0) & (src == 0)))
                def _():
                    remote(recv.at[at], recv.at[at], send_sem.at[0], recv_sem.at[at], sp=me).wait_recv()
        lax.fori_loop(1, n, arrive, None)

        def head(gh, _):
            g, h = lax.div(gh, bn // HEAD), lax.rem(gh, bn // HEAD)
            r, l = pl.ds(pl.multiple_of(g * own, own), own), pl.ds(pl.multiple_of(h * HEAD, HEAD), HEAD)
            for jj in range(n // 2):
                begin, end = max(2 * jj, 1), 2 * jj + 2
                q = recv[pl.ds((p * 3) * n + begin, end - begin), r, l].reshape((end - begin) * own, HEAD)
                k = recv[pl.ds((p * 3 + 1) * n, end), r, l].reshape(end * own, HEAD)
                v = recv[pl.ds((p * 3 + 2) * n, end), r, l].reshape(end * own, HEAD)
                o = attend(q, k, v, begin * own, end * own)
                ostage[pl.ds(p * n + begin, end - begin), r, l] = o.reshape(end - begin, own, HEAD)
        lax.fori_loop(0, 2 * (bn // HEAD), head, None)

        @pl.when(me != 0)
        def _():
            obuf[p, me, c] = ostage[p * n + me]

        def give(i, _):
            to = lax.rem(me + off(i), n)

            @pl.when((to != 0) & (i != 0))
            def _():
                osend(p, to).start()

            @pl.when((to != 0) & (i == 0))
            def _():
                up = upward(3, me).astype(jnp.int32)
                at = (RUNS * 3 + p) * 2 + 1 - up
                remote(ostage.at[p * n + to], via.at[at], osend_sem.at[p * n + to], vrecv_sem.at[at],
                       sp=lax.rem(me + n - quarter + 2 * quarter * up, n)).start()
        lax.fori_loop(0, n - 1, give, None)

    lax.fori_loop(0, RUNS, attention, None)

    for g in range(2):
        acc[g * own : (g + 1) * own, :] = xs[g, :, pl.ds(pl.multiple_of(c * half, half), half)].astype(jnp.float32)

    def forward(t):
        p, src = lax.div(t, n), source(lax.rem(t, n))
        return remote(obuf.at[p, src, c], obuf.at[p, src, c], fsend_sem.at[t], frecv_sem.at[t], dp=mate)

    steps = RUNS * n
    tile = min(512, half)

    def gathered(u):
        p, src = lax.div(u, n), source(lax.rem(u, n))
        slot = lax.rem(u, WO_SLOTS)
        remote(obuf.at[p, src, 1 - c], obuf.at[p, src, 1 - c], fsend_sem.at[u], frecv_sem.at[u], dp=mate).wait_recv()
        pltpu.make_async_copy(wo_ref.at[pl.ds(0, 2 * bn), pl.ds(0, half)], wobuf.at[slot], wo_sem.at[slot]).wait()
        return jnp.concatenate([obuf[p, src, 0], obuf[p, src, 1]], axis=1), slot

    def output(t, _):
        p, i = lax.div(t, n), lax.rem(t, n)

        @pl.when(i == 0)
        def _():
            relay(p, 0, True)

        @pl.when((i != 0) & (me != 0))
        def _():
            src = source(i)
            remote(obuf.at[p, src, c], obuf.at[p, src, c], osend_sem.at[0], orecv_sem.at[p * n + src], sp=me).wait_recv()
        forward(t).start()

        @pl.when(t > 0)
        def _():
            o, slot = gathered(t - 1)

            def columns(k, _):
                here = pl.ds(pl.multiple_of(k * tile, tile), tile)
                acc[:, here] += _dot(o, wobuf[slot, :, here])
            lax.fori_loop(0, half // tile, columns, None)

            @pl.when(t - 1 + WO_SLOTS < steps)
            def _():
                wo_start(t - 1 + WO_SLOTS)

    lax.fori_loop(0, steps, output, None)

    def there(k):
        return out_ref.at[:, pl.ds(pl.multiple_of(c * half + k * tile, tile), tile)]

    def y_give(k):
        return remote(ybuf.at[1 - c, :, pl.ds(pl.multiple_of(k * tile, tile), tile)], there(k), y_sems.at[0, k], y_sems.at[1, k], dp=mate)

    def y_keep(k):
        return pltpu.make_async_copy(ybuf.at[c, :, pl.ds(pl.multiple_of(k * tile, tile), tile)], there(k), y_sems.at[2, k])

    o, slot = gathered(jnp.int32(steps - 1))

    def finish(k, _):
        here = pl.ds(pl.multiple_of(k * tile, tile), tile)
        y = (acc[:, here] + _dot(o, wobuf[slot, :, here])).astype(jnp.bfloat16)
        for g in range(2):
            ybuf[g, :, here] = y[g * own : (g + 1) * own]

        @pl.when(k > 0)
        def _():
            y_give(k - 1).start()
            y_keep(k - 1).start()
    lax.fori_loop(0, half // tile, finish, None)
    y_give(half // tile - 1).start()
    y_keep(half // tile - 1).start()

    swap.wait_send()

    def left(b, _):
        @pl.when(sends(b))
        def _():
            send(b).wait_send()
    lax.fori_loop(blocks - AHEAD, blocks, left, None)

    def vleft(k, _):
        relayed(lax.div(k, 3), lax.rem(k, 3))
    lax.fori_loop(0, RUNS * 3, vleft, None)
    for p in range(RUNS):
        relayed(p, 0, True)

    def oleft(k, _):
        @pl.when((lax.rem(k, n) != me) & (lax.rem(k, n) != 0))
        def _():
            osend(lax.div(k, n), lax.rem(k, n)).wait_send()
        forward(k).wait_send()
    lax.fori_loop(0, steps, oleft, None)

    def yleft(k, _):
        y_give(k).wait_send()
        y_keep(k).wait()
        remote(ybuf.at[c, :, pl.ds(0, tile)], out_ref.at[:, pl.ds(pl.multiple_of((1 - c) * half + k * tile, tile), tile)],
               y_sems.at[0, k], y_sems.at[1, k], dp=mate).wait_recv()
    lax.fori_loop(0, half // tile, yleft, None)


def solution(mesh):
    n = mesh.shape["sp"]

    def step(x, gain, wq, wk, wv, wo):
        own, d = x.shape
        bn = wq.shape[1] // n // 2 // RUNS
        half = HEAD // 2
        place = lax.axis_index("sp") * own + jnp.arange(own)
        angle = place.astype(jnp.float32)[:, None] * THETA ** (-jnp.arange(half, dtype=jnp.float32) / half)
        cos, sin = jnp.cos(angle), jnp.sin(angle)
        cos, sin = jnp.concatenate([cos, cos], -1), jnp.concatenate([-sin, sin], -1)
        blocks, steps = RUNS * 3 * n, RUNS * n
        vmem = pl.BlockSpec(memory_space=pltpu.VMEM)
        hbm = pl.BlockSpec(memory_space=pl.ANY)
        dma, low = pltpu.SemaphoreType.DMA, jnp.bfloat16
        return pl.pallas_call(
            functools.partial(_kernel, n, own),
            out_shape=jax.ShapeDtypeStruct((own, d), low),
            in_specs=[hbm, vmem, vmem, vmem, hbm, hbm, hbm, hbm],
            out_specs=hbm,
            scratch_shapes=[
                pltpu.VMEM((2, own, d), low),
                pltpu.VMEM((2 * own, d), low),
                pltpu.VMEM((SLOTS, d, bn), low),
                pltpu.VMEM((blocks, 2 * own, bn), low),
                pltpu.VMEM((blocks, 2 * own, bn), low),
                pltpu.VMEM((steps, 2 * own, bn), low),
                pltpu.VMEM((RUNS, n, 2, 2 * own, bn), low),
                pltpu.VMEM((WO_SLOTS, 2 * bn, d // 2), low),
                pltpu.VMEM((2 * own, d // 2), jnp.float32),
                pltpu.VMEM((2, own, d // 2), low),
                pltpu.VMEM((2 * (RUNS * 3 + RUNS), 2 * own, bn), low),
                dma((3,)), dma((SLOTS,)), dma((WO_SLOTS,)), dma((blocks,)), dma((blocks,)), dma((steps,)), dma((steps,)),
                dma((steps,)), dma((steps,)), dma((2 * (RUNS * 3 + RUNS),)), dma((2 * (RUNS * 3 + RUNS),)),
                dma((3, d // 2 // min(512, d // 2))),
            ],
            compiler_params=pltpu.CompilerParams(collective_id=0, has_side_effects=True, vmem_limit_bytes=VMEM),
        )(x, jnp.broadcast_to(gain, (16, d)), cos, sin, wq, wk, wv, wo)

    tokens, whole = P(("dp", "sp"), None), P(None, None)
    return jax.shard_map(
        step,
        mesh=mesh,
        in_specs=(tokens, P(None), whole, whole, whole, whole),
        out_specs=tokens,
        check_vma=False,
    )
```

```python
import functools

import jax
import jax.numpy as jnp
from jax import lax
from jax.experimental import pallas as pl
from jax.experimental.pallas import tpu as pltpu
from jax.sharding import PartitionSpec as P

HEAD = 128
THETA = 10000
LOG2E = 1.4426950408889634
HIDDEN = -1e30
SLOTS = 3
WO_SLOTS = 3
AHEAD = 24
RUNS = 2
VMEM = 61 * 2**20


def _dot(a, b, ca=1, cb=0):
    return lax.dot_general(a, b, (((ca,), (cb,)), ((), ())), preferred_element_type=jnp.float32)


def _kernel(n, own, x_ref, gain_ref, cos_ref, sin_ref, wq_ref, wk_ref, wv_ref, wo_ref, out_ref,
            xs, a, wbuf, stage, recv, ostage, obuf, wobuf, acc, ybuf, via,
            x_sems, w_sem, wo_sem, send_sem, recv_sem, osend_sem, orecv_sem, fsend_sem, frecv_sem, vsend_sem, vrecv_sem, y_sems):
    d = x_ref.shape[1]
    half = d // 2
    bn = wbuf.shape[2]
    owner_span = wq_ref.shape[1] // n
    core_span = owner_span // 2
    me = lax.axis_index("sp")
    dp = lax.axis_index("dp")
    c = lax.rem(dp, 2)
    mate = dp + 1 - 2 * c
    blocks = RUNS * 3 * n

    def off(i):
        e = lax.rem(i, 2)
        k = lax.div(i, 2)
        return (1 - e) * (n // 2 - k) + e * (n // 2 + 1 + k)

    def parts(b):
        p = lax.div(b, 3 * n)
        w = lax.div(lax.rem(b, 3 * n), n)
        i = lax.rem(b, n)
        return p, w, i, lax.rem(me + off(i), n)

    rows4 = d // 4

    def w_start(b):
        p, w, _, to = parts(b)
        col = pl.multiple_of(to * owner_span + c * core_span + p * bn, bn)
        slot = lax.rem(b, SLOTS)
        for k, ref in enumerate((wq_ref, wk_ref, wv_ref)):
            @pl.when(w == k)
            def _():
                for r in range(4):
                    pltpu.make_async_copy(ref.at[pl.ds(r * rows4, rows4), pl.ds(col, bn)],
                                          wbuf.at[slot, pl.ds(r * rows4, rows4), :], w_sem.at[slot]).start()

    def w_wait(b):
        slot = lax.rem(b, SLOTS)
        pltpu.make_async_copy(wq_ref.at[:, pl.ds(0, bn)], wbuf.at[slot], w_sem.at[slot]).wait()

    def remote(src, dst, one, two, **to):
        return pltpu.make_async_remote_copy(src, dst, one, two, device_id=to, device_id_type=pl.DeviceIdType.MESH)

    quarter = n // 4

    def half_rows(side):
        return pl.ds(pl.multiple_of(side * own, own), own)

    def send(b, rows=slice(None)):
        p, w, i, to = parts(b)
        at = (p * 3 + w) * n + me
        return remote(stage.at[b, rows], recv.at[at, rows], send_sem.at[b], recv_sem.at[at], sp=to)

    def first_leg(block, group, side, sem):
        at = group * 2 + side
        return remote(block.at[half_rows(side)], via.at[at], sem, vrecv_sem.at[at], sp=lax.rem(me + quarter + (n - 2 * quarter) * side, n))

    def send_start(b, g=None):
        p, w, i, to = parts(b)

        @pl.when((i != 0) & (i != n - 1))
        def _():
            send(b, slice(None) if g is None else half_rows(g)).start()

        @pl.when(i == 0)
        def _():
            for side in range(2) if g is None else (g,):
                first_leg(stage.at[b], p * 3 + w, side, send_sem.at[b]).start()

    def second_leg(p, w, side, result):
        group = RUNS * 3 + p if result else p * 3 + w
        come = lax.rem(me + n - quarter + 2 * quarter * side, n)
        go = lax.rem(me + quarter + (n - 2 * quarter) * side, n)
        at = group * 2 + side
        if result:
            return remote(via.at[at], obuf.at[p, come, c, half_rows(side)], vsend_sem.at[at], orecv_sem.at[p * n + come], sp=go), at
        to = (p * 3 + w) * n + come
        return remote(via.at[at], recv.at[to, half_rows(side)], vsend_sem.at[at], recv_sem.at[to], sp=go), at

    def relay(p, w, result=False):
        for side in range(2):
            on, at = second_leg(p, w, side, result)
            remote(via.at[at], via.at[at], vsend_sem.at[at], vrecv_sem.at[at], sp=me).wait_recv()
            on.start()

    def relayed(p, w, result=False):
        for side in range(2):
            second_leg(p, w, side, result)[0].wait_send()

    for b in range(SLOTS):
        w_start(jnp.int32(b))
    mine = pltpu.make_async_copy(x_ref, xs.at[c], x_sems.at[0])
    mine.start()
    barrier = pltpu.get_barrier_semaphore()
    for s in range(1, n):
        pl.semaphore_signal(barrier, inc=1, device_id={"sp": lax.rem(me + s, n)}, device_id_type=pl.DeviceIdType.MESH)
    pl.semaphore_signal(barrier, inc=1, device_id={"dp": mate}, device_id_type=pl.DeviceIdType.MESH)
    pl.semaphore_wait(barrier, n)
    swap = pltpu.make_async_remote_copy(x_ref, xs.at[c], x_sems.at[1], x_sems.at[2], device_id={"dp": mate},
                                        device_id_type=pl.DeviceIdType.MESH)
    swap.start()

    def norm(g):
        def strip(r, _):
            at = pl.multiple_of(r * 16, 16)
            wide = xs[g, pl.ds(at, 16), :].astype(jnp.float32)
            scale = lax.rsqrt(jnp.mean(wide * wide, -1, keepdims=True) + 1e-6)
            a[pl.ds(pl.multiple_of(g * own + at, 16), 16), :] = (wide * scale * gain_ref[...].astype(jnp.float32)).astype(jnp.bfloat16)
        lax.fori_loop(0, own // 16, strip, None)

    def turned(t, w, rows):
        turn = w < 2
        pieces = []
        for g in range(rows):
            line = []
            for h in range(bn // HEAD):
                u = t[g * own : (g + 1) * own, h * HEAD : (h + 1) * HEAD]
                u = jnp.where(turn, u * cos_ref[...] + pltpu.roll(u, HEAD // 2, 1) * sin_ref[...], u)
                line.append(u.astype(jnp.bfloat16))
            pieces.append(jnp.concatenate(line, axis=1))
        return jnp.concatenate(pieces, axis=0)

    mine.wait()
    norm(c)

    def early_part(k):
        return jnp.where(k < SLOTS, c, 1 - c)

    def early(k, _):
        b, rows = lax.rem(k, SLOTS), half_rows(early_part(k))

        @pl.when(k < SLOTS)
        def _():
            w_wait(b)

        @pl.when(k == SLOTS)
        def _():
            remote(x_ref, xs.at[1 - c], x_sems.at[1], x_sems.at[2], dp=mate).wait_recv()
            norm(1 - c)

        @pl.when(k > 0)
        def _():
            send_start(lax.rem(k - 1, SLOTS), early_part(k - 1))
        _, w, _, _ = parts(b)
        t = _dot(a[rows, :], wbuf[b]).astype(jnp.bfloat16).astype(jnp.float32)

        @pl.when(k >= SLOTS)
        def _():
            w_start(b + SLOTS)
        stage[b, rows, :] = turned(t, w, 1)

    lax.fori_loop(0, 2 * SLOTS, early, None)

    def project(b, _):
        p, w, i, to = parts(b)
        slot = lax.rem(b, SLOTS)
        w_wait(b)

        @pl.when(b == SLOTS)
        def _():
            send_start(b - 1, early_part(2 * SLOTS - 1))

        @pl.when(b > SLOTS)
        def _():
            send_start(b - 1)

        @pl.when((b >= AHEAD) & (lax.rem(b, n) != n - 1))
        def _():
            send(b - AHEAD).wait_send()

        @pl.when((i == n // 2 - 1) & (b >= n))
        def _():
            before = lax.div(b, n) - 1
            relay(lax.div(before, 3), lax.rem(before, 3))

        t = _dot(a[...], wbuf[slot]).astype(jnp.bfloat16).astype(jnp.float32)

        @pl.when(b + SLOTS < blocks)
        def _():
            w_start(b + SLOTS)

        block = turned(t, w, 2)
        stage[b] = block

        @pl.when(i == n - 1)
        def _():
            recv[(p * 3 + w) * n + me] = block

    lax.fori_loop(SLOTS, blocks, project, None)

    def step_of(t):
        near = t < RUNS * (n - 1)
        j = lax.rem(t, n - 1)
        p = jnp.where(near, lax.div(t, n - 1), t - RUNS * (n - 1))
        i = jnp.where(near, jnp.where(j == 0, n - 1, j), 0)
        return p, i, lax.rem(me + n - lax.rem(off(i), n), n)

    def wo_start(t):
        p, _, src = step_of(t)
        slot = lax.rem(t, WO_SLOTS)
        for k in range(2):
            row = pl.multiple_of(src * owner_span + k * core_span + p * bn, bn)
            pltpu.make_async_copy(wo_ref.at[pl.ds(row, bn), pl.ds(pl.multiple_of(c * half, half), half)],
                                  wobuf.at[slot, pl.ds(k * bn, bn), :], wo_sem.at[slot]).start()

    for t in range(WO_SLOTS):
        wo_start(jnp.int32(t))

    relay(RUNS - 1, 2)

    def osend(p, to):
        return remote(ostage.at[p * n + to], obuf.at[p, me, c], osend_sem.at[p * n + to], orecv_sem.at[p * n + me], sp=to)

    e = HEAD**-0.5 * LOG2E

    def attend(q, k, v, first, last):
        s = _dot(k, q, 1, 1)
        queries = q.shape[0]
        shape = (last - first, queries)
        ok = lax.broadcasted_iota(jnp.int32, shape, 1) + (last - queries) >= lax.broadcasted_iota(jnp.int32, shape, 0) + first
        edge = jnp.where(ok, s[first:, :], HIDDEN)
        s = edge if first == 0 else jnp.concatenate([s[:first, :], edge], axis=0)
        top = s.max(axis=0, keepdims=True)
        weights = jnp.exp2((s - top) * e)
        total = weights.sum(axis=0, keepdims=True)
        mix = _dot(v, weights.astype(jnp.bfloat16), 0, 0)
        return (mix * (1 / total)).T.astype(jnp.bfloat16)

    def attention(p, _):
        def arrive(s, _):
            src = lax.rem(me + s, n)
            for w in range(3):
                at = (p * 3 + w) * n + src
                remote(recv.at[at], recv.at[at], send_sem.at[0], recv_sem.at[at], sp=me).wait_recv()
        lax.fori_loop(1, n, arrive, None)

        def head(gh, _):
            g, h = lax.div(gh, bn // HEAD), lax.rem(gh, bn // HEAD)
            r, l = pl.ds(pl.multiple_of(g * own, own), own), pl.ds(pl.multiple_of(h * HEAD, HEAD), HEAD)
            for jj in range(n // 2):
                begin, end = 2 * jj, 2 * jj + 2
                q = recv[pl.ds((p * 3) * n + begin, end - begin), r, l].reshape((end - begin) * own, HEAD)
                k = recv[pl.ds((p * 3 + 1) * n, end), r, l].reshape(end * own, HEAD)
                v = recv[pl.ds((p * 3 + 2) * n, end), r, l].reshape(end * own, HEAD)
                o = attend(q, k, v, begin * own, end * own)
                ostage[pl.ds(p * n + begin, end - begin), r, l] = o.reshape(end - begin, own, HEAD)
        lax.fori_loop(0, 2 * (bn // HEAD), head, None)

        obuf[p, me, c] = ostage[p * n + me]
        for side in range(2):
            to = lax.rem(me + n // 2, n)
            first_leg(ostage.at[p * n + to], RUNS * 3 + p, side, osend_sem.at[p * n + to]).start()

        def give(i, _):
            osend(p, lax.rem(me + off(i), n)).start()
        lax.fori_loop(1, n - 1, give, None)

    lax.fori_loop(0, RUNS, attention, None)

    for g in range(2):
        acc[g * own : (g + 1) * own, :] = xs[g, :, pl.ds(pl.multiple_of(c * half, half), half)].astype(jnp.float32)

    def forward(t):
        p, _, src = step_of(t)
        return remote(obuf.at[p, src, c], obuf.at[p, src, c], fsend_sem.at[t], frecv_sem.at[t], dp=mate)

    steps = RUNS * n
    tile = min(512, half)

    def gathered(u):
        p, _, src = step_of(u)
        slot = lax.rem(u, WO_SLOTS)
        remote(obuf.at[p, src, 1 - c], obuf.at[p, src, 1 - c], fsend_sem.at[u], frecv_sem.at[u], dp=mate).wait_recv()
        pltpu.make_async_copy(wo_ref.at[pl.ds(0, 2 * bn), pl.ds(0, half)], wobuf.at[slot], wo_sem.at[slot]).wait()
        return jnp.concatenate([obuf[p, src, 0], obuf[p, src, 1]], axis=1), slot

    def output(t, _):
        p, i, src = step_of(t)

        @pl.when(lax.rem(t, n) == 0)
        def _():
            relay(lax.div(t, n), 0, True)

        @pl.when(i != n - 1)
        def _():
            remote(obuf.at[p, src, c], obuf.at[p, src, c], osend_sem.at[0], orecv_sem.at[p * n + src], sp=me).wait_recv()
        forward(t).start()

        @pl.when(t > 0)
        def _():
            o, slot = gathered(t - 1)

            def columns(k, _):
                here = pl.ds(pl.multiple_of(k * tile, tile), tile)
                acc[:, here] += _dot(o, wobuf[slot, :, here])
            lax.fori_loop(0, half // tile, columns, None)

            @pl.when(t - 1 + WO_SLOTS < steps)
            def _():
                wo_start(t - 1 + WO_SLOTS)

    lax.fori_loop(0, steps, output, None)

    def there(k):
        return out_ref.at[:, pl.ds(pl.multiple_of(c * half + k * tile, tile), tile)]

    def y_give(k):
        return remote(ybuf.at[:, pl.ds(pl.multiple_of(k * tile, tile), tile)], there(k), y_sems.at[0, k], y_sems.at[1, k], dp=mate)

    o, slot = gathered(jnp.int32(steps - 1))

    def finish(k, _):
        here = pl.ds(pl.multiple_of(k * tile, tile), tile)
        y = (acc[:, here] + _dot(o, wobuf[slot, :, here])).astype(jnp.bfloat16)
        first, second = y[:own], y[own:]
        ybuf[:, here] = jnp.where(c == 0, second, first)
        out_ref[:, pl.ds(pl.multiple_of(c * half + k * tile, tile), tile)] = jnp.where(c == 0, first, second)

        @pl.when(k > 0)
        def _():
            y_give(k - 1).start()
    lax.fori_loop(0, half // tile, finish, None)
    y_give(half // tile - 1).start()

    swap.wait_send()

    def left(b, _):
        @pl.when(lax.rem(b, n) != n - 1)
        def _():
            send(b).wait_send()
    lax.fori_loop(blocks - AHEAD, blocks, left, None)

    def vleft(k, _):
        relayed(lax.div(k, 3), lax.rem(k, 3))
    lax.fori_loop(0, RUNS * 3, vleft, None)
    for p in range(RUNS):
        relayed(p, 0, True)

    def oleft(k, _):
        @pl.when(lax.rem(k, n) != me)
        def _():
            osend(lax.div(k, n), lax.rem(k, n)).wait_send()
        forward(k).wait_send()
    lax.fori_loop(0, steps, oleft, None)

    def yleft(k, _):
        y_give(k).wait_send()
        remote(ybuf.at[:, pl.ds(0, tile)], out_ref.at[:, pl.ds(pl.multiple_of((1 - c) * half + k * tile, tile), tile)],
               y_sems.at[0, k], y_sems.at[1, k], dp=mate).wait_recv()
    lax.fori_loop(0, half // tile, yleft, None)


def solution(mesh):
    n = mesh.shape["sp"]

    def step(x, gain, wq, wk, wv, wo):
        own, d = x.shape
        bn = wq.shape[1] // n // 2 // RUNS
        half = HEAD // 2
        place = lax.axis_index("sp") * own + jnp.arange(own)
        angle = place.astype(jnp.float32)[:, None] * THETA ** (-jnp.arange(half, dtype=jnp.float32) / half)
        cos, sin = jnp.cos(angle), jnp.sin(angle)
        cos, sin = jnp.concatenate([cos, cos], -1), jnp.concatenate([-sin, sin], -1)
        blocks, steps = RUNS * 3 * n, RUNS * n
        vmem = pl.BlockSpec(memory_space=pltpu.VMEM)
        hbm = pl.BlockSpec(memory_space=pl.ANY)
        dma, low = pltpu.SemaphoreType.DMA, jnp.bfloat16
        return pl.pallas_call(
            functools.partial(_kernel, n, own),
            out_shape=pltpu.VMEM((own, d), low),
            in_specs=[hbm, vmem, vmem, vmem, hbm, hbm, hbm, hbm],
            out_specs=vmem,
            scratch_shapes=[
                pltpu.VMEM((2, own, d), low),
                pltpu.VMEM((2 * own, d), low),
                pltpu.VMEM((SLOTS, d, bn), low),
                pltpu.VMEM((blocks, 2 * own, bn), low),
                pltpu.VMEM((blocks, 2 * own, bn), low),
                pltpu.VMEM((steps, 2 * own, bn), low),
                pltpu.VMEM((RUNS, n, 2, 2 * own, bn), low),
                pltpu.VMEM((WO_SLOTS, 2 * bn, d // 2), low),
                pltpu.VMEM((2 * own, d // 2), jnp.float32),
                pltpu.VMEM((own, d // 2), low),
                pltpu.VMEM((2 * (RUNS * 3 + RUNS), own, bn), low),
                dma((3,)), dma((SLOTS,)), dma((WO_SLOTS,)), dma((blocks,)), dma((blocks,)), dma((steps,)), dma((steps,)),
                dma((steps,)), dma((steps,)), dma((2 * (RUNS * 3 + RUNS),)), dma((2 * (RUNS * 3 + RUNS),)),
                dma((2, d // 2 // min(512, d // 2))),
            ],
            compiler_params=pltpu.CompilerParams(collective_id=0, has_side_effects=True, vmem_limit_bytes=VMEM),
        )(x, jnp.broadcast_to(gain, (16, d)), cos, sin, wq, wk, wv, wo)

    tokens, whole = P(("dp", "sp"), None), P(None, None)
    return jax.shard_map(
        step,
        mesh=mesh,
        in_specs=(tokens, P(None), whole, whole, whole, whole),
        out_specs=tokens,
        check_vma=False,
    )
```

```python
import functools

import jax
import jax.numpy as jnp
from jax import lax
from jax.experimental import pallas as pl
from jax.experimental.pallas import tpu as pltpu
from jax.sharding import PartitionSpec as P

HEAD = 128
THETA = 10000
LOG2E = 1.4426950408889634
HIDDEN = -1e30
SLOTS = 3
WO_SLOTS = 3
AHEAD = 24
RUNS = 2
VMEM = 61 * 2**20


def _dot(a, b, ca=1, cb=0):
    return lax.dot_general(a, b, (((ca,), (cb,)), ((), ())), preferred_element_type=jnp.float32)


def _kernel(n, own, x_ref, gain_ref, cos_ref, sin_ref, wq_ref, wk_ref, wv_ref, wo_ref, out_ref,
            xs, a, wbuf, stage, recv, ostage, obuf, wobuf, acc, ybuf, via, hvia,
            x_sems, w_sem, wo_sem, send_sem, recv_sem, osend_sem, orecv_sem, fsend_sem, frecv_sem, vsend_sem, vrecv_sem, hsend_sem, hrecv_sem, y_sems):
    d = x_ref.shape[1]
    half = d // 2
    bn = wbuf.shape[2]
    owner_span = wq_ref.shape[1] // n
    core_span = owner_span // 2
    me = lax.axis_index("sp")
    dp = lax.axis_index("dp")
    c = lax.rem(dp, 2)
    mate = dp + 1 - 2 * c
    blocks = RUNS * 3 * n

    near = 4
    ways = [2, n - 2, 1, n - 1]
    for m in range(3, n // 2):
        ways += [m, n - m]
    ways += [n // 2, n]
    far = n - 2 - near

    def off(i):
        return functools.reduce(lambda found, k: jnp.where(i == k, ways[k], found), range(1, n), jnp.int32(ways[0]))

    def parts(b):
        p = lax.div(b, 3 * n)
        w = lax.div(lax.rem(b, 3 * n), n)
        i = lax.rem(b, n)
        return p, w, i, lax.rem(me + off(i), n)

    rows4 = d // 4

    def w_start(b):
        p, w, _, to = parts(b)
        col = pl.multiple_of(to * owner_span + c * core_span + p * bn, bn)
        slot = lax.rem(b, SLOTS)
        for k, ref in enumerate((wq_ref, wk_ref, wv_ref)):
            @pl.when(w == k)
            def _():
                for r in range(4):
                    pltpu.make_async_copy(ref.at[pl.ds(r * rows4, rows4), pl.ds(col, bn)],
                                          wbuf.at[slot, pl.ds(r * rows4, rows4), :], w_sem.at[slot]).start()

    def w_wait(b):
        slot = lax.rem(b, SLOTS)
        pltpu.make_async_copy(wq_ref.at[:, pl.ds(0, bn)], wbuf.at[slot], w_sem.at[slot]).wait()

    def remote(src, dst, one, two, **to):
        return pltpu.make_async_remote_copy(src, dst, one, two, device_id=to, device_id_type=pl.DeviceIdType.MESH)

    def half_rows(side):
        return pl.ds(pl.multiple_of(side * own, own), own)

    def send(b, rows=slice(None)):
        p, w, i, to = parts(b)
        at = (p * 3 + w) * n + me
        return remote(stage.at[b, rows], recv.at[at, rows], send_sem.at[b], recv_sem.at[at], sp=to)

    def beside(side):
        return lax.rem(me + 1 + (n - 2) * side, n)

    def far_leg(block, group, i, sem):
        at = group * far + i - near
        return remote(block, via.at[at], sem, vrecv_sem.at[at], sp=beside(lax.rem(i - near, 2)))

    def half_leg(block, group, side, sem):
        at = group * 2 + side
        return remote(block.at[half_rows(side)], hvia.at[at], sem, hrecv_sem.at[at], sp=beside(side))

    def send_start(b):
        p, w, i, to = parts(b)

        @pl.when(i < near)
        def _():
            send(b).start()

        @pl.when((i >= near) & (i < n - 2))
        def _():
            far_leg(stage.at[b], p * 3 + w, i, send_sem.at[b]).start()

        @pl.when(i == n - 2)
        def _():
            for side in range(2):
                half_leg(stage.at[b], p * 3 + w, side, send_sem.at[b]).start()

    def passed(p, w, result):
        group = RUNS * 3 + p if result else p * 3 + w
        found = []
        for k in [k for m in range(0, far, 2) for k in (m + 1, m)] + [far + 1, far]:
            side, half_way = k % 2, k >= far
            at = group * 2 + side if half_way else group * far + k
            held, one, two = (hvia, hsend_sem, hrecv_sem) if half_way else (via, vsend_sem, vrecv_sem)
            come = beside(1 - side)
            go = lax.rem(come + (n // 2 if half_way else ways[near + k]), n)
            rows = half_rows(side) if half_way else slice(None)
            if result:
                on = remote(held.at[at], obuf.at[p, come, c, rows], one.at[at], orecv_sem.at[p * n + come], sp=go)
            else:
                to = (p * 3 + w) * n + come
                on = remote(held.at[at], recv.at[to, rows], one.at[at], recv_sem.at[to], sp=go)
            found.append((remote(held.at[at], held.at[at], one.at[at], two.at[at], sp=me), on))
        return found

    def relay(p, w, result=False):
        for came, on in passed(p, w, result):
            came.wait_recv()
            on.start()

    def relayed(p, w, result=False):
        for _, on in passed(p, w, result):
            on.wait_send()

    for b in range(SLOTS):
        w_start(jnp.int32(b))
    mine = pltpu.make_async_copy(x_ref, xs.at[c], x_sems.at[0])
    mine.start()
    barrier = pltpu.get_barrier_semaphore()
    for s in range(1, n):
        pl.semaphore_signal(barrier, inc=1, device_id={"sp": lax.rem(me + s, n)}, device_id_type=pl.DeviceIdType.MESH)
    pl.semaphore_signal(barrier, inc=1, device_id={"dp": mate}, device_id_type=pl.DeviceIdType.MESH)
    pl.semaphore_wait(barrier, n)
    swap = pltpu.make_async_remote_copy(x_ref, xs.at[c], x_sems.at[1], x_sems.at[2], device_id={"dp": mate},
                                        device_id_type=pl.DeviceIdType.MESH)
    swap.start()

    def norm(g):
        def strip(r, _):
            at = pl.multiple_of(r * 16, 16)
            wide = xs[g, pl.ds(at, 16), :].astype(jnp.float32)
            scale = lax.rsqrt(jnp.mean(wide * wide, -1, keepdims=True) + 1e-6)
            a[pl.ds(pl.multiple_of(g * own + at, 16), 16), :] = (wide * scale * gain_ref[...]).astype(jnp.bfloat16)
        lax.fori_loop(0, own // 16, strip, None)

    def turned(t, w, rows):
        turn = w < 2
        pieces = []
        for g in range(rows):
            line = []
            for h in range(bn // HEAD):
                u = t[g * own : (g + 1) * own, h * HEAD : (h + 1) * HEAD]
                u = jnp.where(turn, u * cos_ref[...] + pltpu.roll(u, HEAD // 2, 1) * sin_ref[...], u)
                line.append(u.astype(jnp.bfloat16))
            pieces.append(jnp.concatenate(line, axis=1))
        return jnp.concatenate(pieces, axis=0)

    mine.wait()
    norm(c)

    def early_part(k):
        return jnp.where(k < SLOTS, c, 1 - c)

    def early(k, _):
        b, rows = lax.rem(k, SLOTS), half_rows(early_part(k))

        @pl.when(k < SLOTS)
        def _():
            w_wait(b)

        @pl.when(k == SLOTS)
        def _():
            remote(x_ref, xs.at[1 - c], x_sems.at[1], x_sems.at[2], dp=mate).wait_recv()
            norm(1 - c)

        @pl.when(k > 0)
        def _():
            send(lax.rem(k - 1, SLOTS), half_rows(early_part(k - 1))).start()
        _, w, _, _ = parts(b)
        t = _dot(a[rows, :], wbuf[b]).astype(jnp.bfloat16).astype(jnp.float32)

        @pl.when(k >= SLOTS)
        def _():
            w_start(b + SLOTS)
        stage[b, rows, :] = turned(t, w, 1)

    lax.fori_loop(0, 2 * SLOTS, early, None)

    def project(b, _):
        p, w, i, to = parts(b)
        slot = lax.rem(b, SLOTS)
        w_wait(b)

        @pl.when(b == SLOTS)
        def _():
            send(b - 1, half_rows(early_part(2 * SLOTS - 1))).start()

        @pl.when(b > SLOTS)
        def _():
            send_start(b - 1)

        @pl.when((b >= AHEAD) & (lax.rem(b, n) != n - 1))
        def _():
            send(b - AHEAD).wait_send()

        @pl.when((i == 0) & (b >= n))
        def _():
            before = lax.div(b, n) - 1
            relay(lax.div(before, 3), lax.rem(before, 3))

        t = _dot(a[...], wbuf[slot]).astype(jnp.bfloat16).astype(jnp.float32)

        @pl.when(b + SLOTS < blocks)
        def _():
            w_start(b + SLOTS)

        block = turned(t, w, 2)
        stage[b] = block

        @pl.when(i == n - 1)
        def _():
            recv[(p * 3 + w) * n + me] = block

    lax.fori_loop(SLOTS, blocks, project, None)

    def step_of(t):
        u = jnp.maximum(t - RUNS * (near + 1), 0)
        first = t < RUNS * (near + 1)
        j = lax.rem(t, near + 1)
        p = jnp.where(first, lax.div(t, near + 1), lax.div(u, n - 1 - near))
        i = jnp.where(first, jnp.where(j == 0, n - 1, j - 1), near + lax.rem(u, n - 1 - near))
        return p, i, lax.rem(me + n - lax.rem(off(i), n), n)

    def wo_start(t):
        p, _, src = step_of(t)
        slot = lax.rem(t, WO_SLOTS)
        for k in range(2):
            row = pl.multiple_of(src * owner_span + k * core_span + p * bn, bn)
            pltpu.make_async_copy(wo_ref.at[pl.ds(row, bn), pl.ds(pl.multiple_of(c * half, half), half)],
                                  wobuf.at[slot, pl.ds(k * bn, bn), :], wo_sem.at[slot]).start()

    for t in range(WO_SLOTS):
        wo_start(jnp.int32(t))

    relay(RUNS - 1, 2)

    def osend(p, to):
        return remote(ostage.at[p * n + to], obuf.at[p, me, c], osend_sem.at[p * n + to], orecv_sem.at[p * n + me], sp=to)

    e = HEAD**-0.5 * LOG2E

    def attend(q, k, v, first, last):
        s = _dot(k, q, 1, 1)
        queries = q.shape[0]
        shape = (last - first, queries)
        ok = lax.broadcasted_iota(jnp.int32, shape, 1) + (last - queries) >= lax.broadcasted_iota(jnp.int32, shape, 0) + first
        edge = jnp.where(ok, s[first:, :], HIDDEN)
        s = edge if first == 0 else jnp.concatenate([s[:first, :], edge], axis=0)
        top = s.max(axis=0, keepdims=True)
        weights = jnp.exp2((s - top) * e)
        total = weights.sum(axis=0, keepdims=True)
        mix = _dot(v, weights.astype(jnp.bfloat16), 0, 0)
        return (mix * (1 / total)).T.astype(jnp.bfloat16)

    def attention(p, _):
        def arrive(s, _):
            src = lax.rem(me + s, n)
            for w in range(3):
                at = (p * 3 + w) * n + src
                remote(recv.at[at], recv.at[at], send_sem.at[0], recv_sem.at[at], sp=me).wait_recv()
        lax.fori_loop(1, n, arrive, None)

        def head(gh, _):
            g, h = lax.div(gh, bn // HEAD), lax.rem(gh, bn // HEAD)
            r, l = pl.ds(pl.multiple_of(g * own, own), own), pl.ds(pl.multiple_of(h * HEAD, HEAD), HEAD)
            for jj in range(n // 2):
                begin, end = 2 * jj, 2 * jj + 2
                q = recv[pl.ds((p * 3) * n + begin, end - begin), r, l].reshape((end - begin) * own, HEAD)
                k = recv[pl.ds((p * 3 + 1) * n, end), r, l].reshape(end * own, HEAD)
                v = recv[pl.ds((p * 3 + 2) * n, end), r, l].reshape(end * own, HEAD)
                o = attend(q, k, v, begin * own, end * own)
                ostage[pl.ds(p * n + begin, end - begin), r, l] = o.reshape(end - begin, own, HEAD)
        lax.fori_loop(0, 2 * (bn // HEAD), head, None)

        obuf[p, me, c] = ostage[p * n + me]

        def give(i, _):
            to = lax.rem(me + off(i), n)

            @pl.when(i < near)
            def _():
                osend(p, to).start()

            @pl.when((i >= near) & (i < n - 2))
            def _():
                far_leg(ostage.at[p * n + to], RUNS * 3 + p, i, osend_sem.at[p * n + to]).start()

            @pl.when(i == n - 2)
            def _():
                for side in range(2):
                    half_leg(ostage.at[p * n + to], RUNS * 3 + p, side, osend_sem.at[p * n + to]).start()
        lax.fori_loop(0, n - 1, give, None)

    lax.fori_loop(0, RUNS, attention, None)

    for g in range(2):
        acc[g * own : (g + 1) * own, :] = xs[g, :, pl.ds(pl.multiple_of(c * half, half), half)].astype(jnp.float32)

    def forward(t):
        p, _, src = step_of(t)
        return remote(obuf.at[p, src, c], obuf.at[p, src, c], fsend_sem.at[t], frecv_sem.at[t], dp=mate)

    steps = RUNS * n
    tile = min(512, half)

    def gathered(u):
        p, _, src = step_of(u)
        slot = lax.rem(u, WO_SLOTS)
        remote(obuf.at[p, src, 1 - c], obuf.at[p, src, 1 - c], fsend_sem.at[u], frecv_sem.at[u], dp=mate).wait_recv()
        pltpu.make_async_copy(wo_ref.at[pl.ds(0, 2 * bn), pl.ds(0, half)], wobuf.at[slot], wo_sem.at[slot]).wait()
        return jnp.concatenate([obuf[p, src, 0], obuf[p, src, 1]], axis=1), slot

    def output(t, _):
        p, i, src = step_of(t)

        @pl.when(lax.rem(t, n) == 0)
        def _():
            relay(lax.div(t, n), 0, True)

        @pl.when(i != n - 1)
        def _():
            remote(obuf.at[p, src, c], obuf.at[p, src, c], osend_sem.at[0], orecv_sem.at[p * n + src], sp=me).wait_recv()
        forward(t).start()

        @pl.when(t > 0)
        def _():
            o, slot = gathered(t - 1)

            def columns(k, _):
                here = pl.ds(pl.multiple_of(k * tile, tile), tile)
                acc[:, here] += _dot(o, wobuf[slot, :, here])
            lax.fori_loop(0, half // tile, columns, None)

            @pl.when(t - 1 + WO_SLOTS < steps)
            def _():
                wo_start(t - 1 + WO_SLOTS)

    lax.fori_loop(0, steps, output, None)

    def there(k):
        return out_ref.at[:, pl.ds(pl.multiple_of(c * half + k * tile, tile), tile)]

    def y_give(k):
        return remote(ybuf.at[:, pl.ds(pl.multiple_of(k * tile, tile), tile)], there(k), y_sems.at[0, k], y_sems.at[1, k], dp=mate)

    o, slot = gathered(jnp.int32(steps - 1))

    def finish(k, _):
        here = pl.ds(pl.multiple_of(k * tile, tile), tile)
        y = (acc[:, here] + _dot(o, wobuf[slot, :, here])).astype(jnp.bfloat16)
        first, second = y[:own], y[own:]
        ybuf[:, here] = jnp.where(c == 0, second, first)
        out_ref[:, pl.ds(pl.multiple_of(c * half + k * tile, tile), tile)] = jnp.where(c == 0, first, second)

        @pl.when(k > 0)
        def _():
            y_give(k - 1).start()
    lax.fori_loop(0, half // tile, finish, None)
    y_give(half // tile - 1).start()

    swap.wait_send()

    def left(b, _):
        @pl.when(lax.rem(b, n) != n - 1)
        def _():
            send(b).wait_send()
    lax.fori_loop(blocks - AHEAD, blocks, left, None)

    def vleft(k, _):
        relayed(lax.div(k, 3), lax.rem(k, 3))
    lax.fori_loop(0, RUNS * 3, vleft, None)
    for p in range(RUNS):
        relayed(p, 0, True)

    def oleft(k, _):
        @pl.when(lax.rem(k, n) != me)
        def _():
            osend(lax.div(k, n), lax.rem(k, n)).wait_send()
        forward(k).wait_send()
    lax.fori_loop(0, steps, oleft, None)

    def yleft(k, _):
        y_give(k).wait_send()
        remote(ybuf.at[:, pl.ds(0, tile)], out_ref.at[:, pl.ds(pl.multiple_of((1 - c) * half + k * tile, tile), tile)],
               y_sems.at[0, k], y_sems.at[1, k], dp=mate).wait_recv()
    lax.fori_loop(0, half // tile, yleft, None)


def solution(mesh):
    n = mesh.shape["sp"]

    def step(x, gain, wq, wk, wv, wo):
        own, d = x.shape
        bn = wq.shape[1] // n // 2 // RUNS
        half = HEAD // 2
        place = lax.axis_index("sp") * own + jnp.arange(own)
        angle = place.astype(jnp.float32)[:, None] * THETA ** (-jnp.arange(half, dtype=jnp.float32) / half)
        cos, sin = jnp.cos(angle), jnp.sin(angle)
        cos, sin = jnp.concatenate([cos, cos], -1), jnp.concatenate([-sin, sin], -1)
        blocks, steps, groups = RUNS * 3 * n, RUNS * n, RUNS * 4
        vmem = pl.BlockSpec(memory_space=pltpu.VMEM)
        hbm = pl.BlockSpec(memory_space=pl.ANY)
        dma, low = pltpu.SemaphoreType.DMA, jnp.bfloat16
        return pl.pallas_call(
            functools.partial(_kernel, n, own),
            out_shape=pltpu.VMEM((own, d), low),
            in_specs=[hbm, vmem, vmem, vmem, hbm, hbm, hbm, hbm],
            out_specs=vmem,
            scratch_shapes=[
                pltpu.VMEM((2, own, d), low),
                pltpu.VMEM((2 * own, d), low),
                pltpu.VMEM((SLOTS, d, bn), low),
                pltpu.VMEM((blocks, 2 * own, bn), low),
                pltpu.VMEM((blocks, 2 * own, bn), low),
                pltpu.VMEM((steps, 2 * own, bn), low),
                pltpu.VMEM((RUNS, n, 2, 2 * own, bn), low),
                pltpu.VMEM((WO_SLOTS, 2 * bn, d // 2), low),
                pltpu.VMEM((2 * own, d // 2), jnp.float32),
                pltpu.VMEM((own, d // 2), low),
                pltpu.VMEM((groups * (n - 6), 2 * own, bn), low),
                pltpu.VMEM((groups * 2, own, bn), low),
                dma((3,)), dma((SLOTS,)), dma((WO_SLOTS,)), dma((blocks,)), dma((blocks,)), dma((steps,)), dma((steps,)),
                dma((steps,)), dma((steps,)), dma((groups * (n - 6),)), dma((groups * (n - 6),)), dma((groups * 2,)), dma((groups * 2,)),
                dma((2, d // 2 // min(512, d // 2))),
            ],
            compiler_params=pltpu.CompilerParams(collective_id=0, has_side_effects=True, vmem_limit_bytes=VMEM),
        )(x, gain.astype(jnp.float32).reshape(1, d), cos, sin, wq, wk, wv, wo)

    tokens, whole = P(("dp", "sp"), None), P(None, None)
    return jax.shard_map(
        step,
        mesh=mesh,
        in_specs=(tokens, P(None), whole, whole, whole, whole),
        out_specs=tokens,
        check_vma=False,
    )
```
